128 devices in a mesh: pair: 32 (over y, z, x_hi), aux: 4 (over x_lo, core).
Axes of the slice: x: 4 (x_hi: 2, x_lo: 2; x = x_hi * 2 + x_lo), y: 4, z: 4, core: 2. Of those that a mesh axis runs over, the one named last changes fastest.
Arguments:
- pair_factors: bfloat16 [65536, 16384], P('pair', 'aux'), may hold values from -0.048913987 to 0.048913987
- pair_weights: float32 [65536], P('pair'), may hold values from 0.08 to 0.8
- probes: float32 [16384, 64], P('aux'), may hold values from -12 to 12
Outputs:
- last_vectors: float32 [16384, 64], P('aux', 'pair')
- moments: float32 [9], replicated
- energy: float32 [1], replicated
The draws below stay inside these ranges and needn't reach their ends.
All inputs are finite; a program needn't handle non-finite values.
Results may differ from the reference program's by a relative error of at most 0.019.
Values may be sent and summed in bfloat16 or wider, within the bound.
A program may use at most 64 MiB of HBM per device.

```python
import math
import jax
import jax.numpy as jnp
import numpy as np
from jax import lax

AUXDIM = 16384
NPROBE = 64
ITERS = 8
PAIRS = 65536


def draw_pair_factors(key, part):
    scale = 1.0 / jnp.sqrt(jnp.float32(PAIRS + AUXDIM))
    scale_key = jax.random.fold_in(key, 7)
    base_key = jax.random.fold_in(key, 11)
    log_square = jax.random.uniform(scale_key, (AUXDIM,), jnp.float32, jnp.log(0.3), jnp.log(12.0))
    column_norm = jnp.exp(0.5 * log_square)
    base = jax.random.truncated_normal(base_key, -4.0, 4.0, (PAIRS, AUXDIM), jnp.float32)
    return (base * column_norm[None, :] * scale).astype(jnp.bfloat16)


def draw_probes(key, part):
    column = jnp.arange(NPROBE, dtype=jnp.float32) / (NPROBE - 1)
    base = jax.random.truncated_normal(key, -4.0, 4.0, (AUXDIM, NPROBE), jnp.float32)
    scale = jnp.exp(column * 0.5 * jnp.log(9.0))
    return base * scale[None, :]


def shard_levels(stream_key, extent, cuts, least, top_value):
    gain = 1.0
    for axis_at, parts in cuts:
        heights = jax.random.uniform(jax.random.fold_in(jax.random.fold_in(stream_key, 6), axis_at), (parts,), jnp.float32, least / len(cuts), top_value / len(cuts))
        gain = gain * jnp.repeat(jnp.exp(heights), extent[axis_at] // parts).reshape((-1,) + (1,) * (len(extent) - 1 - axis_at))
    return gain


def setup_inputs(seed: int = 0) -> dict:
    key_of = jax.random.split(jax.random.key(seed), 4)
    return {
        "pair_factors": draw_pair_factors(jax.random.fold_in(key_of[3], 71), 0),
        "pair_weights": jnp.clip(jnp.exp(math.log(0.8) - 2.3025851 * jax.random.uniform(key_of[1], (PAIRS,), jnp.float32) ** shard_levels(key_of[1], (PAIRS,), ((0, 32),), -0.2, 0.2)), 0.08, 0.8),
        "probes": draw_probes(jax.random.fold_in(key_of[3], 71), 0),
    }


spread = 5.0


def cheb_coefficients(order_count):
    node_count = 64
    angles = (np.arange(node_count) + 0.5) * np.pi / node_count
    samples = np.log(1.0 + spread * (np.cos(angles) + 1.0) / 2.0)
    values = [2.0 / node_count * np.sum(samples * np.cos(degree * angles)) for degree in range(order_count)]
    values[0] = values[0] / 2.0
    return np.array(values)


def reference(pair_factors, pair_weights, probes):
    divisor = NPROBE * AUXDIM
    previous = probes
    current = probes
    moment_list = [jnp.sum(probes * current) / divisor]
    for degree in range(ITERS):
        rows = jnp.dot(pair_factors, current.astype(jnp.bfloat16), preferred_element_type=jnp.float32)
        scaled = (pair_weights[:, None] * rows).astype(jnp.bfloat16)
        image = lax.dot_general(pair_factors, scaled, (((0,), (0,)), ((), ())), preferred_element_type=jnp.float32)
        mapped = (2.0 / spread) * image - current
        following = mapped if degree == 0 else 2.0 * mapped - previous
        previous, current = current, following
        moment_list.append(jnp.sum(probes * current) / divisor)
    moments = jnp.stack(moment_list).astype(jnp.float32)
    coefficients = jnp.asarray(cheb_coefficients(ITERS + 1)).astype(moments.dtype)
    energy = jnp.sum(coefficients * moments).reshape(1)
    return current, moments, energy
```

```python
import jax
import jax.numpy as jnp
import numpy as np
from jax import lax
from jax.experimental import pallas as pl
from jax.experimental.pallas import tpu as pltpu
from jax.sharding import Mesh
from jax.sharding import PartitionSpec as P

ITERS = 8
AUX = ("aux_0", "aux_1")
PAIR = ("pair_0", "pair_1", "pair_2")
MESH_ID = pl.DeviceIdType.MESH
F32 = jnp.float32
BF16 = jnp.bfloat16

spread = 5.0

ROWS = 2048
COLS = 4096
NP = 64
HALF = 2
PEERS = 16
LANES = 128
NCH = 4
RCH = ROWS // NCH
RH = RCH // 2

OFFSETS = (
    (2, 2), (2, 1), (2, 3), (1, 2), (3, 2), (1, 1), (3, 3), (1, 3),
    (3, 1), (2, 0), (0, 2), (1, 0), (0, 1), (3, 0), (0, 3),
)


def cheb_coefficients(order_count):
    node_count = 64
    angles = (np.arange(node_count) + 0.5) * np.pi / node_count
    samples = np.log(1.0 + spread * (np.cos(angles) + 1.0) / 2.0)
    values = [
        2.0 / node_count * np.sum(samples * np.cos(degree * angles))
        for degree in range(order_count)
    ]
    values[0] = values[0] / 2.0
    return np.array(values)


def kernel(
    b_hbm, w_ref, z_hbm, out_ref, mom_out,
    bmat, bt, zbuf, vg, racc, own_half, asend, arecv, bsend, brecv, sbuf,
    rssend, rsrecv, xsend, xrecv, prob, prev, cur, finsend, finrecv, mom, momrecv, momx,
    load_sem, a_s, a_r, b_s, b_r, c_s, c_r, rs_s, rs_r, x_s, x_r, ag_s, ag_r, f_s, f_r, m_s, m_r, q_s, q_r,
):
    y = lax.axis_index("pair_0")
    z = lax.axis_index("pair_1")
    h = lax.axis_index("pair_2")
    xl = lax.axis_index("aux_0")
    core = lax.axis_index("aux_1")
    me = y * 4 + z

    def peer(dy, dz):
        return {"pair_0": lax.rem(y + dy, 4), "pair_1": lax.rem(z + dz, 4)}

    def peer_index(dy, dz):
        return lax.rem(y + dy, 4) * 4 + lax.rem(z + dz, 4)

    hi_id = {"pair_2": 1 - h}
    lo_id = {"aux_0": 1 - xl}
    core_id = {"aux_1": 1 - core}
    diag_id = {"aux_0": 1 - xl, "aux_1": 1 - core}

    loads = [
        pltpu.make_async_copy(
            b_hbm.at[pl.ds(r * 256, 256)], bmat.at[pl.ds(r * 256, 256)], load_sem.at[r]
        )
        for r in range(ROWS // 256)
    ]
    zload = pltpu.make_async_copy(z_hbm, zbuf, load_sem.at[ROWS // 256])
    zload.start()
    for ld in loads:
        ld.start()

    barrier = pltpu.get_barrier_semaphore()
    everyone = [peer(dy, dz) for dy, dz in OFFSETS] + [hi_id, lo_id, core_id, diag_id]
    for who in everyone:
        pl.semaphore_signal(barrier, inc=1, device_id=who, device_id_type=MESH_ID)

    def rcopy(src, dst, s, r, who):
        return pltpu.make_async_remote_copy(
            src_ref=src, dst_ref=dst, send_sem=s, recv_sem=r, device_id=who, device_id_type=MESH_ID
        )

    def wait_bytes(ref, sem):
        pltpu.make_async_copy(ref, ref, sem).wait()

    zload.wait()
    for c in range(HALF):
        def put(p, carry, c=c):
            blk = zbuf[pl.ds(c * 2048 + p * LANES, LANES), :]
            vg[c, p] = blk.T.astype(BF16)
            return carry
        lax.fori_loop(0, PEERS, put, 0)
        blk = zbuf[pl.ds(c * 2048 + me * LANES, LANES), :].T
        prob[c] = blk
        cur[c] = blk
        prev[c] = blk
    mom[...] = jnp.zeros_like(mom)
    mom[0:1, :] = jnp.sum(prob[0] * prob[0] + prob[1] * prob[1], axis=0, keepdims=True)

    for r in range(ROWS // 256):
        loads[r].wait()

        def flip(k, carry, r=r):
            bt[pl.ds(k * 256, 256), r * 256:(r + 1) * 256] = bmat[
                r * 256:(r + 1) * 256, pl.ds(k * 256, 256)
            ].T
            return carry

        lax.fori_loop(0, COLS // 256, flip, 0)

    pl.semaphore_wait(barrier, len(everyone))

    def vector(c):
        return jnp.concatenate([vg[c, p] for p in range(PEERS)], axis=1)

    def step(t, carry):
        par = lax.rem(t, 2)

        @pl.when(t > 0)
        def _():
            wait_bytes(vg.at[0, pl.ds(0, PEERS - 1)], ag_r.at[0])

        for i in range(NCH):
            racc[i] = jnp.dot(
                vector(0), bt[0:2048, i * RCH:(i + 1) * RCH], preferred_element_type=F32
            )

        @pl.when(t > 0)
        def _():
            wait_bytes(vg.at[1, pl.ds(0, PEERS - 1)], ag_r.at[1])
            for c in range(HALF):
                wait_bytes(vg.at[c, pl.ds(0, PEERS - 1)], ag_s.at[c])

        acopy = [
            rcopy(asend.at[i], arecv.at[i], a_s.at[i], a_r.at[i], core_id) for i in range(NCH)
        ]
        bcopy = [
            rcopy(bsend.at[i], brecv.at[par, i], b_s.at[i], b_r.at[par, i], lo_id)
            for i in range(NCH)
        ]
        ccopy = [
            rcopy(
                sbuf.at[2 * i + core], sbuf.at[2 * i + core], c_s.at[i], c_r.at[i], core_id
            )
            for i in range(NCH)
        ]

        def first(i):
            part = racc[i] + jnp.dot(
                vector(1), bt[2048:4096, i * RCH:(i + 1) * RCH], preferred_element_type=F32
            )
            low, high = part[:, :RH], part[:, RH:]
            own_half[i] = jnp.where(core == 0, low, high)
            asend[i] = jnp.where(core == 0, high, low).astype(BF16)
            acopy[i].start()

        def second(i):
            acopy[i].wait_recv()
            bsend[i] = (own_half[i] + arecv[i].astype(F32)).astype(BF16)
            bcopy[i].start()

        def third(i):
            bcopy[i].wait_recv()
            total = bsend[i].astype(F32) + brecv[par, i].astype(F32)
            sbuf[2 * i + core] = (w_ref[2 * i + core] * total).astype(BF16)
            ccopy[i].start()

        first(0)
        first(1)
        first(2)
        second(0)
        first(3)
        second(1)
        second(2)
        second(3)
        for i in range(NCH):
            third(i)
        for i in range(NCH):
            ccopy[i].wait_recv()
            acopy[i].wait_send()
            bcopy[i].wait_send()
            ccopy[i].wait_send()

        scaled = lambda: jnp.concatenate([sbuf[q] for q in range(2 * NCH)], axis=1)
        for c in range(HALF):
            for n in range(4):
                col = c * 2048 + n * 512
                img = jnp.dot(
                    scaled(), bmat[:, col:col + 512], preferred_element_type=F32
                ).astype(BF16)
                for q in range(4):
                    rssend[c, n * 4 + q] = img[:, q * LANES:(q + 1) * LANES]
            for dy, dz in OFFSETS:
                rcopy(
                    rssend.at[c, peer_index(dy, dz)], rsrecv.at[c, me],
                    rs_s.at[c], rs_r.at[c], peer(dy, dz),
                ).start()
            rsrecv[c, me] = rssend[c, me]

        xcopy = [
            rcopy(xsend.at[c], xrecv.at[par, c], x_s.at[c], x_r.at[par, c], hi_id)
            for c in range(HALF)
        ]
        for c in range(HALF):
            wait_bytes(rsrecv.at[c, pl.ds(0, PEERS - 1)], rs_r.at[c])
            total = rsrecv[c, 0].astype(F32)
            for p in range(1, PEERS):
                total = total + rsrecv[c, p].astype(F32)
            xsend[c] = total.astype(BF16)
            xcopy[c].start()

        gain = jnp.where(t == 0, 1.0, 2.0).astype(F32)
        back = jnp.where(t == 0, 0.0, 1.0).astype(F32)
        for c in range(HALF):
            xcopy[c].wait_recv()
            image = xsend[c].astype(F32) + xrecv[par, c].astype(F32)
            now = cur[c]
            mapped = (2.0 / spread) * image - now
            following = gain * mapped - back * prev[c]
            prev[c] = now
            cur[c] = following

            @pl.when(t < ITERS - 1)
            def _(c=c, following=following):
                vg[c, me] = following.astype(BF16)
                for dy, dz in OFFSETS:
                    rcopy(
                        vg.at[c, me], vg.at[c, me], ag_s.at[c], ag_r.at[c], peer(dy, dz)
                    ).start()

        mom[pl.ds(t + 1, 1), :] = jnp.sum(
            prob[0] * cur[0] + prob[1] * cur[1], axis=0, keepdims=True
        )
        for c in range(HALF):
            xcopy[c].wait_send()
            wait_bytes(rssend.at[c, pl.ds(0, PEERS - 1)], rs_s.at[c])
        return carry

    lax.fori_loop(0, ITERS, step, 0)

    momrecv[me] = mom[...]
    for dy, dz in OFFSETS:
        rcopy(mom, momrecv.at[me], m_s, m_r, peer(dy, dz)).start()
    for p in range(PEERS):
        for c in range(HALF):
            four = cur[c, 4 * p:4 * p + 4, :]
            finsend[p, 2 * c:2 * c + 2, :] = jnp.where(h == 0, four[0:2], four[2:4])
    for dy, dz in OFFSETS:
        rcopy(finsend.at[peer_index(dy, dz)], finrecv.at[me], f_s, f_r, peer(dy, dz)).start()
    finrecv[me] = finsend[me]

    wait_bytes(momrecv.at[pl.ds(0, PEERS - 1)], m_r)
    total = momrecv[0]
    for p in range(1, PEERS):
        total = total + momrecv[p]
    slot = xl * 2 + core
    momx[slot] = total
    for who in (core_id, lo_id, diag_id):
        rcopy(momx.at[slot], momx.at[slot], q_s, q_r, who).start()
    wait_bytes(finrecv.at[pl.ds(0, PEERS - 1)], f_r)
    out_ref[...] = finrecv[...]
    wait_bytes(momx.at[pl.ds(0, 3)], q_r)
    mom_out[...] = (momx[0] + momx[1]) + (momx[2] + momx[3])
    wait_bytes(momrecv.at[pl.ds(0, PEERS - 1)], m_s)
    wait_bytes(finsend.at[pl.ds(0, PEERS - 1)], f_s)
    wait_bytes(momx.at[pl.ds(0, 3)], q_s)


def per_device(pair_factors, pair_weights, probes):
    vm = pltpu.VMEM
    dma = pltpu.SemaphoreType.DMA
    out, mom = pl.pallas_call(
        kernel,
        out_shape=(
            jax.ShapeDtypeStruct((PEERS, 4, LANES), F32),
            jax.ShapeDtypeStruct((16, LANES), F32),
        ),
        in_specs=[
            pl.BlockSpec(memory_space=pl.ANY),
            pl.BlockSpec(memory_space=pltpu.VMEM),
            pl.BlockSpec(memory_space=pl.ANY),
        ],
        out_specs=(
            pl.BlockSpec(memory_space=pltpu.VMEM),
            pl.BlockSpec(memory_space=pltpu.VMEM),
        ),
        scratch_shapes=[
            vm((ROWS, COLS), BF16),
            vm((COLS, ROWS), BF16),
            vm((COLS, NP), F32),
            vm((HALF, PEERS, NP, LANES), BF16),
            vm((NCH, NP, RCH), F32),
            vm((NCH, NP, RH), F32),
            vm((NCH, NP, RH), BF16),
            vm((NCH, NP, RH), BF16),
            vm((NCH, NP, RH), BF16),
            vm((2, NCH, NP, RH), BF16),
            vm((2 * NCH, NP, RH), BF16),
            vm((HALF, PEERS, NP, LANES), BF16),
            vm((HALF, PEERS, NP, LANES), BF16),
            vm((HALF, NP, LANES), BF16),
            vm((2, HALF, NP, LANES), BF16),
            vm((HALF, NP, LANES), F32),
            vm((HALF, NP, LANES), F32),
            vm((HALF, NP, LANES), F32),
            vm((PEERS, 4, LANES), F32),
            vm((PEERS, 4, LANES), F32),
            vm((16, LANES), F32),
            vm((PEERS, 16, LANES), F32),
            vm((4, 16, LANES), F32),
            dma((ROWS // 256 + 1,)),
            dma((NCH,)), dma((NCH,)),
            dma((NCH,)), dma((2, NCH)),
            dma((NCH,)), dma((NCH,)),
            dma((HALF,)), dma((HALF,)),
            dma((HALF,)), dma((2, HALF)),
            dma((HALF,)), dma((HALF,)),
            dma, dma, dma, dma, dma, dma,
        ],
        compiler_params=pltpu.CompilerParams(
            collective_id=0, has_side_effects=True, vmem_limit_bytes=60 * 1024 * 1024
        ),
        name="cheb",
    )(pair_factors, pair_weights.reshape(2 * NCH, 1, RH), probes)
    own = out.reshape(PEERS, HALF, 2, LANES).transpose(1, 0, 3, 2).reshape(COLS, 2)
    divisor = NP * COLS * lax.axis_size(AUX)
    moments = jnp.sum(mom, axis=1)[: ITERS + 1] / divisor
    coefficients = jnp.asarray(cheb_coefficients(ITERS + 1)).astype(moments.dtype)
    energy = jnp.sum(coefficients * moments).reshape(1)
    return (own, moments, energy)


def solution(mesh):
    torus = Mesh(
        mesh.devices.reshape(4, 4, 2, 2, 2), ("pair_0", "pair_1", "pair_2", "aux_0", "aux_1")
    )
    return jax.shard_map(
        per_device,
        mesh=torus,
        in_specs=(P(PAIR, AUX), P(PAIR), P(AUX, None)),
        out_specs=(P(AUX, PAIR), P(), P()),
        check_vma=False,
    )
```

```python
import jax
import jax.numpy as jnp
import numpy as np
from jax import lax
from jax.experimental import pallas as pl
from jax.experimental.pallas import tpu as pltpu
from jax.sharding import Mesh
from jax.sharding import PartitionSpec as P

ITERS = 8
AUX = ("aux_0", "aux_1")
PAIR = ("pair_0", "pair_1", "pair_2")
MESH_ID = pl.DeviceIdType.MESH
F32 = jnp.float32
BF16 = jnp.bfloat16

spread = 5.0

ROWS = 2048
COLS = 4096
NP = 64
CH = 4
WIDE = COLS // CH
TILES = WIDE // 128
PR = NP // 2
PEERS = 16
LANES = 128
NCH = 4
RCH = ROWS // NCH
RH = RCH // 2

OFFSETS = (
    (2, 2), (2, 1), (2, 3), (1, 2), (3, 2), (1, 1), (3, 3), (1, 3),
    (3, 1), (2, 0), (0, 2), (1, 0), (0, 1), (3, 0), (0, 3),
)

FAR = ((0, 2), (0, 1), (0, 3), (1, 2), (0, 0), (1, 1), (1, 3), (1, 0))
NEAR = ((1, 2), (1, 1), (1, 3), (0, 2), (1, 0), (0, 1), (0, 3))


def cheb_coefficients(order_count):
    node_count = 64
    angles = (np.arange(node_count) + 0.5) * np.pi / node_count
    samples = np.log(1.0 + spread * (np.cos(angles) + 1.0) / 2.0)
    values = [
        2.0 / node_count * np.sum(samples * np.cos(degree * angles))
        for degree in range(order_count)
    ]
    values[0] = values[0] / 2.0
    return np.array(values)


def kernel(
    b_hbm, w_ref, z_hbm, out_ref, mom_out, energy_out,
    bmat, bt, zbuf, vg, racc, own_half, asend, arecv, bsend, brecv, sbuf,
    rssend, rsrecv, xsend, xrecv, prob, prev, cur, finsend, finrecv, mom, momrecv, momx,
    load_sem, a_s, a_r, b_s, b_r, c_s, c_r, rs_s, rs_r, x_s, x_r, ag_s, ag_r, f_s, f_r, m_s, m_r, q_s, q_r,
):
    y = lax.axis_index("pair_0")
    z = lax.axis_index("pair_1")
    h = lax.axis_index("pair_2")
    xl = lax.axis_index("aux_0")
    core = lax.axis_index("aux_1")
    me = y * 4 + z

    def peer(dy, dz):
        return {"pair_0": lax.rem(y + dy, 4), "pair_1": lax.rem(z + dz, 4)}

    def peer_index(dy, dz):
        return lax.rem(y + dy, 4) * 4 + lax.rem(z + dz, 4)

    hi_id = {"pair_2": 1 - h}
    lo_id = {"aux_0": 1 - xl}
    core_id = {"aux_1": 1 - core}
    diag_id = {"aux_0": 1 - xl, "aux_1": 1 - core}

    loads = [
        pltpu.make_async_copy(
            b_hbm.at[pl.ds(r * 256, 256)], bmat.at[pl.ds(r * 256, 256)], load_sem.at[r]
        )
        for r in range(ROWS // 256)
    ]
    zload = pltpu.make_async_copy(z_hbm, zbuf, load_sem.at[ROWS // 256])
    loads[0].start()
    zload.start()
    for ld in loads[1:]:
        ld.start()

    barrier = pltpu.get_barrier_semaphore()
    everyone = [peer(dy, dz) for dy, dz in OFFSETS] + [hi_id, lo_id, core_id, diag_id]
    for who in everyone:
        pl.semaphore_signal(barrier, inc=1, device_id=who, device_id_type=MESH_ID)

    def rcopy(src, dst, s, r, who):
        return pltpu.make_async_remote_copy(
            src_ref=src, dst_ref=dst, send_sem=s, recv_sem=r, device_id=who, device_id_type=MESH_ID
        )

    def wait_bytes(ref, sem):
        pltpu.make_async_copy(ref, ref, sem).wait()

    def flip_rows(r):
        loads[r].wait()

        def flip(k, carry):
            bt[pl.ds(k * 256, 256), r * 256:(r + 1) * 256] = bmat[
                r * 256:(r + 1) * 256, pl.ds(k * 256, 256)
            ].T
            return carry

        lax.fori_loop(0, COLS // 256, flip, 0)

    flip_rows(0)
    zload.wait()
    for j in range(CH):
        for p in range(PEERS):
            col = (j * TILES + p // 2) * LANES
            vg[j, p] = zbuf[PR * (p % 2):PR * (p % 2) + PR, col:col + LANES].astype(BF16)
        blk = zbuf[
            pl.ds(pl.multiple_of(PR * lax.rem(me, 2), PR), PR),
            pl.ds(pl.multiple_of((j * TILES + me // 2) * LANES, LANES), LANES),
        ]
        prob[j] = blk
        cur[j] = blk
        prev[j] = blk

    def dots():
        acc = prob[0] * cur[0]
        for j in range(1, CH):
            acc = acc + prob[j] * cur[j]
        return jnp.sum(acc, axis=0, keepdims=True)

    mom[...] = jnp.zeros_like(mom)
    mom[0:1, :] = dots()
    for r in range(1, ROWS // 256):
        flip_rows(r)

    pl.semaphore_wait(barrier, len(everyone))

    def vector(j):
        return jnp.concatenate(
            [
                jnp.concatenate([vg[j, 2 * k], vg[j, 2 * k + 1]], axis=0)
                for k in range(TILES)
            ],
            axis=1,
        )

    def step(t, carry):
        par = lax.rem(t, 2)

        def rows_part(j, i):
            return jnp.dot(
                vector(j),
                bt[j * WIDE:(j + 1) * WIDE, i * RCH:(i + 1) * RCH],
                preferred_element_type=F32,
            )

        for j in range(CH):
            @pl.when(t > 0)
            def _(j=j):
                wait_bytes(vg.at[j, pl.ds(0, PEERS - 1)], ag_r.at[j])

            if j == CH - 1:
                break
            for i in range(NCH):
                part = rows_part(j, i)
                racc[i] = part if j == 0 else racc[i] + part

        acopy = [
            rcopy(asend.at[i], arecv.at[i], a_s.at[i], a_r.at[i], core_id) for i in range(NCH)
        ]
        bcopy = [
            rcopy(bsend.at[i], brecv.at[par, i], b_s.at[i], b_r.at[par, i], lo_id)
            for i in range(NCH)
        ]
        ccopy = [
            rcopy(
                sbuf.at[2 * i + core], sbuf.at[2 * i + core], c_s.at[i], c_r.at[i], core_id
            )
            for i in range(NCH)
        ]

        def first(i):
            part = racc[i] + rows_part(CH - 1, i)
            low, high = part[:, :RH], part[:, RH:]
            own_half[i] = jnp.where(core == 0, low, high)
            asend[i] = jnp.where(core == 0, high, low).astype(BF16)
            acopy[i].start()

        def second(i):
            acopy[i].wait_recv()
            bsend[i] = (own_half[i] + arecv[i].astype(F32)).astype(BF16)
            bcopy[i].start()

        def third(i):
            bcopy[i].wait_recv()
            total = bsend[i].astype(F32) + brecv[par, i].astype(F32)
            sbuf[2 * i + core] = (w_ref[2 * i + core] * total).astype(BF16)
            ccopy[i].start()

        for i in range(NCH):
            first(i)
        for i in range(NCH):
            second(i)

        @pl.when(t > 0)
        def _():
            for j in range(CH):
                wait_bytes(vg.at[j, pl.ds(0, PEERS - 1)], ag_s.at[j])

        for i in range(NCH):
            third(i)
        for i in range(NCH):
            ccopy[i].wait_recv()

        def scaled():
            return jnp.concatenate([sbuf[q] for q in range(2 * NCH)], axis=1)

        far = 1 - y // 2
        for j in range(CH):
            for k in range(2):
                side = far if k == 0 else 1 - far
                col = pl.multiple_of(j * WIDE + side * 512, 512)
                img = jnp.dot(
                    scaled(), bmat[:, pl.ds(col, 512)], preferred_element_type=F32
                ).astype(BF16)
                for q in range(4):
                    for g in range(2):
                        rssend[j, side * 8 + 2 * q + g] = img[
                            g * PR:(g + 1) * PR, q * LANES:(q + 1) * LANES
                        ]
                order = FAR if k == 0 else NEAR
                for dy, dz in order:
                    ty = 2 * side + lax.rem(y + dy, 2)
                    tz = lax.rem(z + dz, 4)
                    rcopy(
                        rssend.at[j, ty * 4 + tz], rsrecv.at[j, me],
                        rs_s.at[j], rs_r.at[j], {"pair_0": ty, "pair_1": tz},
                    ).start()
            rsrecv[j, me] = rssend[j, me]

        for i in range(NCH):
            acopy[i].wait_send()
            bcopy[i].wait_send()
            ccopy[i].wait_send()

        xcopy = [
            rcopy(xsend.at[j], xrecv.at[par, j], x_s.at[j], x_r.at[par, j], hi_id)
            for j in range(CH)
        ]
        for j in range(CH):
            wait_bytes(rsrecv.at[j, pl.ds(0, PEERS - 1)], rs_r.at[j])
            total = rsrecv[j, 0].astype(F32)
            for p in range(1, PEERS):
                total = total + rsrecv[j, p].astype(F32)
            xsend[j] = total.astype(BF16)
            xcopy[j].start()

        gain = jnp.where(t == 0, 1.0, 2.0).astype(F32)
        back = jnp.where(t == 0, 0.0, 1.0).astype(F32)
        for j in range(CH):
            xcopy[j].wait_recv()
            image = xsend[j].astype(F32) + xrecv[par, j].astype(F32)
            now = cur[j]
            mapped = (2.0 / spread) * image - now
            following = gain * mapped - back * prev[j]
            prev[j] = now
            cur[j] = following

            @pl.when(t < ITERS - 1)
            def _(j=j, following=following):
                vg[j, me] = following.astype(BF16)
                for dy, dz in OFFSETS:
                    rcopy(
                        vg.at[j, me], vg.at[j, me], ag_s.at[j], ag_r.at[j], peer(dy, dz)
                    ).start()

        mom[pl.ds(t + 1, 1), :] = dots()
        for j in range(CH):
            xcopy[j].wait_send()
            wait_bytes(rssend.at[j, pl.ds(0, PEERS - 1)], rs_s.at[j])
        return carry

    lax.fori_loop(0, ITERS, step, 0)

    momrecv[me] = mom[...]
    for dy, dz in OFFSETS:
        rcopy(mom, momrecv.at[me], m_s, m_r, peer(dy, dz)).start()
    for q in range(8):
        for j in range(CH):
            four = cur[j, 4 * q:4 * q + 4, :]
            finsend[q, 2 * j:2 * j + 2, :] = jnp.where(h == 0, four[0:2], four[2:4])
    for dy, dz in OFFSETS:
        rcopy(
            finsend.at[lax.rem(peer_index(dy, dz), 8)], finrecv.at[me], f_s, f_r, peer(dy, dz)
        ).start()
    finrecv[me] = finsend[lax.rem(me, 8)]

    wait_bytes(momrecv.at[pl.ds(0, PEERS - 1)], m_r)
    total = momrecv[0]
    for p in range(1, PEERS):
        total = total + momrecv[p]
    slot = xl * 2 + core
    momx[slot] = total
    for who in (core_id, lo_id, diag_id):
        rcopy(momx.at[slot], momx.at[slot], q_s, q_r, who).start()
    wait_bytes(finrecv.at[pl.ds(0, PEERS - 1)], f_r)
    half = me // 8
    for k in range(TILES):
        for j in range(CH):
            col = (j * TILES + k) * LANES
            out_ref[:, col:col + LANES] = finrecv[2 * k + half, 2 * j:2 * j + 2, :]
    wait_bytes(momx.at[pl.ds(0, 3)], q_r)
    moments = jnp.sum(
        (momx[0] + momx[1]) + (momx[2] + momx[3]), axis=1, keepdims=True
    ) * (1.0 / (NP * COLS * 4))
    energy = jnp.zeros((), F32)
    for k, c in enumerate(cheb_coefficients(ITERS + 1)):
        mom_out[k] = moments[k, 0]
        energy = energy + moments[k, 0] * float(c)
    energy_out[0] = energy
    wait_bytes(momrecv.at[pl.ds(0, PEERS - 1)], m_s)
    wait_bytes(finrecv.at[pl.ds(0, PEERS - 1)], f_s)
    wait_bytes(momx.at[pl.ds(0, 3)], q_s)


def per_device(pair_factors, pair_weights, probes):
    vm = pltpu.VMEM
    dma = pltpu.SemaphoreType.DMA
    out, moments, energy = pl.pallas_call(
        kernel,
        out_shape=(
            jax.ShapeDtypeStruct((2, COLS), F32),
            jax.ShapeDtypeStruct((ITERS + 1,), F32),
            jax.ShapeDtypeStruct((1,), F32),
        ),
        in_specs=[
            pl.BlockSpec(memory_space=pl.ANY),
            pl.BlockSpec(memory_space=pltpu.VMEM),
            pl.BlockSpec(memory_space=pl.ANY),
        ],
        out_specs=(
            pl.BlockSpec(memory_space=pltpu.VMEM),
            pl.BlockSpec(memory_space=pltpu.SMEM),
            pl.BlockSpec(memory_space=pltpu.SMEM),
        ),
        scratch_shapes=[
            vm((ROWS, COLS), BF16),
            vm((COLS, ROWS), BF16),
            vm((NP, COLS), F32),
            vm((CH, PEERS, PR, LANES), BF16),
            vm((NCH, NP, RCH), F32),
            vm((NCH, NP, RH), F32),
            vm((NCH, NP, RH), BF16),
            vm((NCH, NP, RH), BF16),
            vm((NCH, NP, RH), BF16),
            vm((2, NCH, NP, RH), BF16),
            vm((2 * NCH, NP, RH), BF16),
            vm((CH, PEERS, PR, LANES), BF16),
            vm((CH, PEERS, PR, LANES), BF16),
            vm((CH, PR, LANES), BF16),
            vm((2, CH, PR, LANES), BF16),
            vm((CH, PR, LANES), F32),
            vm((CH, PR, LANES), F32),
            vm((CH, PR, LANES), F32),
            vm((8, 2 * CH, LANES), F32),
            vm((PEERS, 2 * CH, LANES), F32),
            vm((16, LANES), F32),
            vm((PEERS, 16, LANES), F32),
            vm((4, 16, LANES), F32),
            dma((ROWS // 256 + 1,)),
            dma((NCH,)), dma((NCH,)),
            dma((NCH,)), dma((2, NCH)),
            dma((NCH,)), dma((NCH,)),
            dma((CH,)), dma((CH,)),
            dma((CH,)), dma((2, CH)),
            dma((CH,)), dma((CH,)),
            dma, dma, dma, dma, dma, dma,
        ],
        compiler_params=pltpu.CompilerParams(
            collective_id=0, has_side_effects=True, vmem_limit_bytes=60 * 1024 * 1024
        ),
        name="cheb",
    )(pair_factors, pair_weights.reshape(2 * NCH, 1, RH), probes.T)
    return (out.T, moments, energy)


def solution(mesh):
    torus = Mesh(
        mesh.devices.reshape(4, 4, 2, 2, 2), ("pair_0", "pair_1", "pair_2", "aux_0", "aux_1")
    )
    return jax.shard_map(
        per_device,
        mesh=torus,
        in_specs=(P(PAIR, AUX), P(PAIR), P(AUX, None)),
        out_specs=(P(AUX, PAIR), P(), P()),
        check_vma=False,
    )
```

```python
import jax
import jax.numpy as jnp
import numpy as np
from jax import lax
from jax.experimental import pallas as pl
from jax.experimental.pallas import tpu as pltpu
from jax.sharding import Mesh
from jax.sharding import PartitionSpec as P

ITERS = 8
AUX = ("aux_0", "aux_1")
PAIR = ("pair_0", "pair_1", "pair_2")
MESH_ID = pl.DeviceIdType.MESH
F32 = jnp.float32
BF16 = jnp.bfloat16

spread = 5.0

ROWS = 2048
COLS = 4096
NP = 64
CH = 2
WIDE = COLS // CH
TILES = WIDE // 128
OWNERS = 32
PARTS = OWNERS // TILES
PR = NP // PARTS
PEERS = 32
LANES = 128
NCH = 4
RCH = ROWS // NCH
RH = RCH // 2

PLANE = (
    (2, 2), (2, 1), (2, 3), (1, 2), (3, 2), (1, 1), (3, 3), (1, 3),
    (3, 1), (2, 0), (0, 2), (1, 0), (0, 1), (3, 0), (0, 3), (0, 0),
)
OFFSETS = tuple((dy, dz, 1) for dy, dz in PLANE) + tuple((dy, dz, 0) for dy, dz in PLANE[:-1])
ZH = ((2, 1), (1, 1), (3, 1), (2, 0), (0, 1), (1, 0), (3, 0), (0, 0))


def cheb_coefficients(order_count):
    node_count = 64
    angles = (np.arange(node_count) + 0.5) * np.pi / node_count
    samples = np.log(1.0 + spread * (np.cos(angles) + 1.0) / 2.0)
    values = [
        2.0 / node_count * np.sum(samples * np.cos(degree * angles))
        for degree in range(order_count)
    ]
    values[0] = values[0] / 2.0
    return np.array(values)


def kernel(
    b_hbm, w_ref, z_hbm, out_ref, mom_out, energy_out,
    bmat, bt, zbuf, vg, racc, own_half, asend, arecv, bsend, brecv, sbuf,
    rssend, rsrecv, prob, prev, cur, finsend, finrecv, mom, momrecv, momx,
    load_sem, a_s, a_r, b_s, b_r, c_s, c_r, rs_s, rs_r, ag_s, ag_r, f_s, f_r, m_s, m_r, q_s, q_r,
):
    y = lax.axis_index("pair_0")
    z = lax.axis_index("pair_1")
    h = lax.axis_index("pair_2")
    xl = lax.axis_index("aux_0")
    core = lax.axis_index("aux_1")
    me = (y * 4 + z) * 2 + h

    def peer(dy, dz, dh):
        return {
            "pair_0": lax.rem(y + dy, 4), "pair_1": lax.rem(z + dz, 4), "pair_2": lax.rem(h + dh, 2)
        }

    def peer_index(dy, dz, dh):
        return (lax.rem(y + dy, 4) * 4 + lax.rem(z + dz, 4)) * 2 + lax.rem(h + dh, 2)

    lo_id = {"aux_0": 1 - xl}
    core_id = {"aux_1": 1 - core}
    diag_id = {"aux_0": 1 - xl, "aux_1": 1 - core}

    loads = [
        pltpu.make_async_copy(
            b_hbm.at[pl.ds(r * 256, 256)], bmat.at[pl.ds(r * 256, 256)], load_sem.at[r]
        )
        for r in range(ROWS // 256)
    ]
    zload = pltpu.make_async_copy(z_hbm, zbuf, load_sem.at[ROWS // 256])
    loads[0].start()
    zload.start()
    for ld in loads[1:]:
        ld.start()

    barrier = pltpu.get_barrier_semaphore()
    everyone = [peer(*off) for off in OFFSETS] + [lo_id, core_id, diag_id]
    for who in everyone:
        pl.semaphore_signal(barrier, inc=1, device_id=who, device_id_type=MESH_ID)

    def rcopy(src, dst, s, r, who):
        return pltpu.make_async_remote_copy(
            src_ref=src, dst_ref=dst, send_sem=s, recv_sem=r, device_id=who, device_id_type=MESH_ID
        )

    def wait_bytes(ref, sem):
        pltpu.make_async_copy(ref, ref, sem).wait()

    def flip_rows(r):
        loads[r].wait()

        def flip(k, carry):
            bt[pl.ds(k * 256, 256), r * 256:(r + 1) * 256] = bmat[
                r * 256:(r + 1) * 256, pl.ds(k * 256, 256)
            ].T
            return carry

        lax.fori_loop(0, COLS // 256, flip, 0)

    flip_rows(0)
    zload.wait()
    for j in range(CH):
        for p in range(PEERS):
            col = (j * TILES + p // PARTS) * LANES
            row = PR * (p % PARTS)
            vg[j, p] = zbuf[row:row + PR, col:col + LANES].astype(BF16)
        blk = zbuf[
            pl.ds(pl.multiple_of(PR * lax.rem(me, PARTS), PR), PR),
            pl.ds(pl.multiple_of((j * TILES + me // PARTS) * LANES, LANES), LANES),
        ]
        prob[j] = blk
        cur[j] = blk
        prev[j] = blk

    def dots():
        acc = prob[0] * cur[0]
        for j in range(1, CH):
            acc = acc + prob[j] * cur[j]
        return jnp.sum(acc, axis=0, keepdims=True)

    mom[...] = jnp.zeros_like(mom)
    mom[0:1, :] = dots()
    for r in range(1, ROWS // 256):
        flip_rows(r)

    pl.semaphore_wait(barrier, len(everyone))

    def vector(j):
        return jnp.concatenate(
            [
                jnp.concatenate([vg[j, PARTS * k + g] for g in range(PARTS)], axis=0)
                for k in range(TILES)
            ],
            axis=1,
        )

    def step(t, carry):
        par = lax.rem(t, 2)

        def rows_part(j, i):
            return jnp.dot(
                vector(j),
                bt[j * WIDE:(j + 1) * WIDE, i * RCH:(i + 1) * RCH],
                preferred_element_type=F32,
            )

        for j in range(CH):
            @pl.when(t > 0)
            def _(j=j):
                wait_bytes(vg.at[j, pl.ds(0, PEERS - 1)], ag_r.at[j])

            if j == CH - 1:
                break
            for i in range(NCH):
                part = rows_part(j, i)
                racc[i] = part if j == 0 else racc[i] + part

        acopy = [
            rcopy(asend.at[i], arecv.at[i], a_s.at[i], a_r.at[i], core_id) for i in range(NCH)
        ]
        bcopy = [
            rcopy(bsend.at[i], brecv.at[par, i], b_s.at[i], b_r.at[par, i], lo_id)
            for i in range(NCH)
        ]
        ccopy = [
            rcopy(
                sbuf.at[2 * i + core], sbuf.at[2 * i + core], c_s.at[i], c_r.at[i], core_id
            )
            for i in range(NCH)
        ]

        def first(i):
            part = racc[i] + rows_part(CH - 1, i)
            low, high = part[:, :RH], part[:, RH:]
            own_half[i] = jnp.where(core == 0, low, high)
            asend[i] = jnp.where(core == 0, high, low).astype(BF16)
            acopy[i].start()

        def second(i):
            acopy[i].wait_recv()
            bsend[i] = (own_half[i] + arecv[i].astype(F32)).astype(BF16)
            bcopy[i].start()

        def third(i):
            bcopy[i].wait_recv()
            total = bsend[i].astype(F32) + brecv[par, i].astype(F32)
            sbuf[2 * i + core] = (w_ref[2 * i + core] * total).astype(BF16)
            ccopy[i].start()

        for i in range(NCH):
            first(i)
        for i in range(NCH):
            second(i)

        @pl.when(t > 0)
        def _():
            for j in range(CH):
                wait_bytes(vg.at[j, pl.ds(0, PEERS - 1)], ag_s.at[j])

        for i in range(NCH):
            third(i)
        for i in range(NCH):
            ccopy[i].wait_recv()

        def scaled():
            return jnp.concatenate([sbuf[q] for q in range(2 * NCH)], axis=1)

        for j in range(CH):
            for k in range(TILES // 4):
                if CH == 2:
                    side = lax.rem(y + (2, 1, 3, 0)[k], 4)
                    ys = [side]
                else:
                    side = (1 - y // 2) if k == 0 else y // 2
                    low = lax.rem(y, 2)
                    ys = [2 * side + low, 2 * side + 1 - low]
                    ys = ys if k == 0 else ys[::-1]
                col = pl.multiple_of(j * WIDE + side * 512, 512)
                img = jnp.dot(
                    scaled(), bmat[:, pl.ds(col, 512)], preferred_element_type=F32
                ).astype(BF16)
                for q in range(4):
                    for g in range(PARTS):
                        rssend[j, (side * 4 + q) * PARTS + g] = img[
                            g * PR:(g + 1) * PR, q * LANES:(q + 1) * LANES
                        ]
                for m, ty in enumerate(ys):
                    own = k == TILES // 4 - 1 and m == len(ys) - 1
                    for dz, dh in ZH[:7] if own else ZH:
                        tz = lax.rem(z + dz, 4)
                        th = lax.rem(h + dh, 2)
                        rcopy(
                            rssend.at[j, (ty * 4 + tz) * 2 + th], rsrecv.at[j, me],
                            rs_s.at[j], rs_r.at[j], {"pair_0": ty, "pair_1": tz, "pair_2": th},
                        ).start()
            rsrecv[j, me] = rssend[j, me]

        for i in range(NCH):
            acopy[i].wait_send()
            bcopy[i].wait_send()
            ccopy[i].wait_send()

        gain = jnp.where(t == 0, 1.0, 2.0).astype(F32)
        back = jnp.where(t == 0, 0.0, 1.0).astype(F32)
        for j in range(CH):
            wait_bytes(rsrecv.at[j, pl.ds(0, PEERS - 1)], rs_r.at[j])
            image = rsrecv[j, 0].astype(F32)
            for p in range(1, PEERS):
                image = image + rsrecv[j, p].astype(F32)
            now = cur[j]
            mapped = (2.0 / spread) * image - now
            following = gain * mapped - back * prev[j]
            prev[j] = now
            cur[j] = following

            @pl.when(t < ITERS - 1)
            def _(j=j, following=following):
                vg[j, me] = following.astype(BF16)
                for off in OFFSETS:
                    rcopy(
                        vg.at[j, me], vg.at[j, me], ag_s.at[j], ag_r.at[j], peer(*off)
                    ).start()

        mom[pl.ds(t + 1, 1), :] = dots()
        for j in range(CH):
            wait_bytes(rssend.at[j, pl.ds(0, PEERS - 1)], rs_s.at[j])
        return carry

    lax.fori_loop(0, ITERS, step, 0)

    momrecv[me] = mom[...]
    for off in OFFSETS:
        rcopy(mom, momrecv.at[me], m_s, m_r, peer(*off)).start()
    for q in range(PR // 2):
        for j in range(CH):
            finsend[q, 2 * j:2 * j + 2, :] = cur[j, 2 * q:2 * q + 2, :]
    for off in OFFSETS:
        rcopy(
            finsend.at[lax.rem(peer_index(*off), PR // 2)], finrecv.at[me], f_s, f_r, peer(*off)
        ).start()
    finrecv[me] = finsend[lax.rem(me, PR // 2)]

    wait_bytes(momrecv.at[pl.ds(0, PEERS - 1)], m_r)
    total = momrecv[0]
    for p in range(1, PEERS):
        total = total + momrecv[p]
    slot = xl * 2 + core
    momx[slot] = total
    for who in (core_id, lo_id, diag_id):
        rcopy(momx.at[slot], momx.at[slot], q_s, q_r, who).start()
    wait_bytes(finrecv.at[pl.ds(0, PEERS - 1)], f_r)
    part = me // (PR // 2)
    for k in range(TILES):
        for j in range(CH):
            col = (j * TILES + k) * LANES
            out_ref[:, col:col + LANES] = finrecv[PARTS * k + part, 2 * j:2 * j + 2, :]
    wait_bytes(momx.at[pl.ds(0, 3)], q_r)
    moments = jnp.sum(
        (momx[0] + momx[1]) + (momx[2] + momx[3]), axis=1, keepdims=True
    ) * (1.0 / (NP * COLS * 4))
    energy = jnp.zeros((), F32)
    for k, c in enumerate(cheb_coefficients(ITERS + 1)):
        mom_out[k] = moments[k, 0]
        energy = energy + moments[k, 0] * float(c)
    energy_out[0] = energy
    wait_bytes(momrecv.at[pl.ds(0, PEERS - 1)], m_s)
    wait_bytes(finrecv.at[pl.ds(0, PEERS - 1)], f_s)
    wait_bytes(momx.at[pl.ds(0, 3)], q_s)


def per_device(pair_factors, pair_weights, probes):
    vm = pltpu.VMEM
    dma = pltpu.SemaphoreType.DMA
    out, moments, energy = pl.pallas_call(
        kernel,
        out_shape=(
            jax.ShapeDtypeStruct((2, COLS), F32),
            jax.ShapeDtypeStruct((ITERS + 1,), F32),
            jax.ShapeDtypeStruct((1,), F32),
        ),
        in_specs=[
            pl.BlockSpec(memory_space=pl.ANY),
            pl.BlockSpec(memory_space=pltpu.VMEM),
            pl.BlockSpec(memory_space=pl.ANY),
        ],
        out_specs=(
            pl.BlockSpec(memory_space=pltpu.VMEM),
            pl.BlockSpec(memory_space=pltpu.SMEM),
            pl.BlockSpec(memory_space=pltpu.SMEM),
        ),
        scratch_shapes=[
            vm((ROWS, COLS), BF16),
            vm((COLS, ROWS), BF16),
            vm((NP, COLS), F32),
            vm((CH, PEERS, PR, LANES), BF16),
            vm((NCH, NP, RCH), F32),
            vm((NCH, NP, RH), F32),
            vm((NCH, NP, RH), BF16),
            vm((NCH, NP, RH), BF16),
            vm((NCH, NP, RH), BF16),
            vm((2, NCH, NP, RH), BF16),
            vm((2 * NCH, NP, RH), BF16),
            vm((CH, PEERS, PR, LANES), BF16),
            vm((CH, PEERS, PR, LANES), BF16),
            vm((CH, PR, LANES), F32),
            vm((CH, PR, LANES), F32),
            vm((CH, PR, LANES), F32),
            vm((PR // 2, 2 * CH, LANES), F32),
            vm((PEERS, 2 * CH, LANES), F32),
            vm((16, LANES), F32),
            vm((PEERS, 16, LANES), F32),
            vm((4, 16, LANES), F32),
            dma((ROWS // 256 + 1,)),
            dma((NCH,)), dma((NCH,)),
            dma((NCH,)), dma((2, NCH)),
            dma((NCH,)), dma((NCH,)),
            dma((CH,)), dma((CH,)),
            dma((CH,)), dma((CH,)),
            dma, dma, dma, dma, dma, dma,
        ],
        compiler_params=pltpu.CompilerParams(
            collective_id=0, has_side_effects=True, vmem_limit_bytes=60 * 1024 * 1024
        ),
        name="cheb",
    )(pair_factors, pair_weights.reshape(2 * NCH, 1, RH), probes.T)
    return (out.T, moments, energy)


def solution(mesh):
    torus = Mesh(
        mesh.devices.reshape(4, 4, 2, 2, 2), ("pair_0", "pair_1", "pair_2", "aux_0", "aux_1")
    )
    return jax.shard_map(
        per_device,
        mesh=torus,
        in_specs=(P(PAIR, AUX), P(PAIR), P(AUX, None)),
        out_specs=(P(AUX, PAIR), P(), P()),
        check_vma=False,
    )
```

```python
import jax
import jax.numpy as jnp
import numpy as np
from jax import lax
from jax.experimental import pallas as pl
from jax.experimental.pallas import tpu as pltpu
from jax.sharding import Mesh
from jax.sharding import PartitionSpec as P

ITERS = 8
AUX = ("aux_0", "aux_1")
PAIR = ("pair_0", "pair_1", "pair_2")
MESH_ID = pl.DeviceIdType.MESH
F32 = jnp.float32
BF16 = jnp.bfloat16

spread = 5.0

ROWS = 2048
COLS = 4096
NP = 64
CH = 4
WIDE = COLS // CH
TILES = WIDE // 128
OWNERS = 32
PARTS = OWNERS // TILES
PR = NP // PARTS
PEERS = 32
LANES = 128
NCH = 4
RCH = ROWS // NCH
RH = RCH // 2

PLANE = (
    (2, 2), (2, 1), (2, 3), (1, 2), (3, 2), (1, 1), (3, 3), (1, 3),
    (3, 1), (2, 0), (0, 2), (1, 0), (0, 1), (3, 0), (0, 3), (0, 0),
)
OFFSETS = tuple((dy, dz, 1) for dy, dz in PLANE) + tuple((dy, dz, 0) for dy, dz in PLANE[:-1])
ZH = ((2, 1), (1, 1), (3, 1), (2, 0), (0, 1), (1, 0), (3, 0), (0, 0))


def cheb_coefficients(order_count):
    node_count = 64
    angles = (np.arange(node_count) + 0.5) * np.pi / node_count
    samples = np.log(1.0 + spread * (np.cos(angles) + 1.0) / 2.0)
    values = [
        2.0 / node_count * np.sum(samples * np.cos(degree * angles))
        for degree in range(order_count)
    ]
    values[0] = values[0] / 2.0
    return np.array(values)


def kernel(
    b_hbm, w_ref, z_hbm, out_ref, mom_out, energy_out,
    bmat, bt, zbuf, vg, racc, own_half, asend, arecv, bsend, brecv, sbuf,
    rssend, rsrecv, prob, prev, cur, finsend, finrecv, mom, momrecv, momx,
    load_sem, a_s, a_r, b_s, b_r, c_s, c_r, rs_s, rs_r, ag_s, ag_r, f_s, f_r, m_s, m_r, q_s, q_r,
):
    y = lax.axis_index("pair_0")
    z = lax.axis_index("pair_1")
    h = lax.axis_index("pair_2")
    xl = lax.axis_index("aux_0")
    core = lax.axis_index("aux_1")
    me = (y * 4 + z) * 2 + h

    def peer(dy, dz, dh):
        return {
            "pair_0": lax.rem(y + dy, 4), "pair_1": lax.rem(z + dz, 4), "pair_2": lax.rem(h + dh, 2)
        }

    def peer_index(dy, dz, dh):
        return (lax.rem(y + dy, 4) * 4 + lax.rem(z + dz, 4)) * 2 + lax.rem(h + dh, 2)

    lo_id = {"aux_0": 1 - xl}
    core_id = {"aux_1": 1 - core}
    diag_id = {"aux_0": 1 - xl, "aux_1": 1 - core}

    loads = [
        pltpu.make_async_copy(
            b_hbm.at[pl.ds(r * 256, 256)], bmat.at[pl.ds(r * 256, 256)], load_sem.at[r]
        )
        for r in range(ROWS // 256)
    ]
    zload = pltpu.make_async_copy(z_hbm, zbuf, load_sem.at[ROWS // 256])
    loads[0].start()
    zload.start()
    for ld in loads[1:]:
        ld.start()

    barrier = pltpu.get_barrier_semaphore()
    everyone = [peer(*off) for off in OFFSETS] + [lo_id, core_id, diag_id]
    for who in everyone:
        pl.semaphore_signal(barrier, inc=1, device_id=who, device_id_type=MESH_ID)

    def rcopy(src, dst, s, r, who):
        return pltpu.make_async_remote_copy(
            src_ref=src, dst_ref=dst, send_sem=s, recv_sem=r, device_id=who, device_id_type=MESH_ID
        )

    def wait_bytes(ref, sem):
        pltpu.make_async_copy(ref, ref, sem).wait()

    def flip_rows(r):
        loads[r].wait()

        def flip(k, carry):
            bt[pl.ds(k * 256, 256), r * 256:(r + 1) * 256] = bmat[
                r * 256:(r + 1) * 256, pl.ds(k * 256, 256)
            ].T
            return carry

        lax.fori_loop(0, COLS // 256, flip, 0, unroll=4)

    flip_rows(0)
    zload.wait()
    for j in range(CH):
        for p in range(PEERS):
            col = (j * TILES + p // PARTS) * LANES
            row = PR * (p % PARTS)
            vg[j, p] = zbuf[row:row + PR, col:col + LANES].astype(BF16)
        blk = zbuf[
            pl.ds(pl.multiple_of(PR * lax.rem(me, PARTS), PR), PR),
            pl.ds(pl.multiple_of((j * TILES + me // PARTS) * LANES, LANES), LANES),
        ]
        prob[j] = blk
        cur[j] = blk
        prev[j] = blk

    def dots():
        acc = prob[0] * cur[0]
        for j in range(1, CH):
            acc = acc + prob[j] * cur[j]
        return jnp.sum(acc, axis=0, keepdims=True)

    mom[...] = jnp.zeros_like(mom)
    mom[0:1, :] = dots()
    for r in range(1, ROWS // 256):
        flip_rows(r)

    pl.semaphore_wait(barrier, len(everyone))

    def vector(j):
        return jnp.concatenate(
            [
                jnp.concatenate([vg[j, PARTS * k + g] for g in range(PARTS)], axis=0)
                for k in range(TILES)
            ],
            axis=1,
        )

    def step(t, carry):
        par = lax.rem(t, 2)

        def rows_part(j, i):
            return jnp.dot(
                vector(j),
                bt[j * WIDE:(j + 1) * WIDE, i * RCH:(i + 1) * RCH],
                preferred_element_type=F32,
            )

        for j in range(CH):
            @pl.when(t > 0)
            def _(j=j):
                wait_bytes(vg.at[j, pl.ds(0, PEERS - 1)], ag_r.at[j])

            if j == CH - 1:
                break
            for i in range(NCH):
                part = rows_part(j, i)
                racc[i] = part if j == 0 else racc[i] + part

        acopy = [
            rcopy(asend.at[i], arecv.at[i], a_s.at[i], a_r.at[i], core_id) for i in range(NCH)
        ]
        bcopy = [
            rcopy(bsend.at[i], brecv.at[par, i], b_s.at[i], b_r.at[par, i], lo_id)
            for i in range(NCH)
        ]
        ccopy = [
            rcopy(
                sbuf.at[2 * i + core], sbuf.at[2 * i + core], c_s.at[i], c_r.at[i], core_id
            )
            for i in range(NCH)
        ]

        def first(i):
            part = racc[i] + rows_part(CH - 1, i)
            low, high = part[:, :RH], part[:, RH:]
            own_half[i] = jnp.where(core == 0, low, high)
            asend[i] = jnp.where(core == 0, high, low).astype(BF16)
            acopy[i].start()

        def second(i):
            acopy[i].wait_recv()
            bsend[i] = (own_half[i] + arecv[i].astype(F32)).astype(BF16)
            bcopy[i].start()

        def third(i):
            bcopy[i].wait_recv()
            total = bsend[i].astype(F32) + brecv[par, i].astype(F32)
            sbuf[2 * i + core] = (w_ref[2 * i + core] * total).astype(BF16)
            ccopy[i].start()

        for i in range(NCH):
            first(i)
        for i in range(NCH):
            second(i)

        @pl.when(t > 0)
        def _():
            for j in range(CH):
                wait_bytes(vg.at[j, pl.ds(0, PEERS - 1)], ag_s.at[j])

        for i in range(NCH):
            third(i)
        for i in range(NCH):
            ccopy[i].wait_recv()

        def scaled():
            return jnp.concatenate([sbuf[q] for q in range(2 * NCH)], axis=1)

        for j in range(CH):
            for k in range(TILES // 4):
                if CH == 2:
                    side = lax.rem(y + (2, 1, 3, 0)[k], 4)
                    ys = [side]
                else:
                    side = (1 - y // 2) if k == 0 else y // 2
                    low = lax.rem(y, 2)
                    ys = [2 * side + low, 2 * side + 1 - low]
                    ys = ys if k == 0 else ys[::-1]
                col = pl.multiple_of(j * WIDE + side * 512, 512)
                img = jnp.dot(
                    scaled(), bmat[:, pl.ds(col, 512)], preferred_element_type=F32
                ).astype(BF16)
                for q in range(4):
                    for g in range(PARTS):
                        rssend[j, (side * 4 + q) * PARTS + g] = img[
                            g * PR:(g + 1) * PR, q * LANES:(q + 1) * LANES
                        ]
                for m, ty in enumerate(ys):
                    own = k == TILES // 4 - 1 and m == len(ys) - 1
                    for dz, dh in ZH[:7] if own else ZH:
                        tz = lax.rem(z + dz, 4)
                        th = lax.rem(h + dh, 2)
                        rcopy(
                            rssend.at[j, (ty * 4 + tz) * 2 + th], rsrecv.at[j, me],
                            rs_s.at[j], rs_r.at[j], {"pair_0": ty, "pair_1": tz, "pair_2": th},
                        ).start()
            rsrecv[j, me] = rssend[j, me]

        for i in range(NCH):
            acopy[i].wait_send()
            bcopy[i].wait_send()
            ccopy[i].wait_send()

        gain = jnp.where(t == 0, 1.0, 2.0).astype(F32)
        back = jnp.where(t == 0, 0.0, 1.0).astype(F32)
        for j in range(CH):
            wait_bytes(rsrecv.at[j, pl.ds(0, PEERS - 1)], rs_r.at[j])
            image = rsrecv[j, 0].astype(F32)
            for p in range(1, PEERS):
                image = image + rsrecv[j, p].astype(F32)
            now = cur[j]
            mapped = (2.0 / spread) * image - now
            following = gain * mapped - back * prev[j]
            prev[j] = now
            cur[j] = following

            @pl.when(t < ITERS - 1)
            def _(j=j, following=following):
                vg[j, me] = following.astype(BF16)
                for off in OFFSETS:
                    rcopy(
                        vg.at[j, me], vg.at[j, me], ag_s.at[j], ag_r.at[j], peer(*off)
                    ).start()

        mom[pl.ds(t + 1, 1), :] = dots()
        for j in range(CH):
            wait_bytes(rssend.at[j, pl.ds(0, PEERS - 1)], rs_s.at[j])
        return carry

    lax.fori_loop(0, ITERS, step, 0)

    momrecv[me] = mom[...]
    for off in OFFSETS:
        rcopy(mom, momrecv.at[me], m_s, m_r, peer(*off)).start()
    for q in range(PR // 2):
        for j in range(CH):
            finsend[q, 2 * j:2 * j + 2, :] = cur[j, 2 * q:2 * q + 2, :]
    for off in OFFSETS:
        rcopy(
            finsend.at[lax.rem(peer_index(*off), PR // 2)], finrecv.at[me], f_s, f_r, peer(*off)
        ).start()
    finrecv[me] = finsend[lax.rem(me, PR // 2)]

    wait_bytes(momrecv.at[pl.ds(0, PEERS - 1)], m_r)
    total = momrecv[0]
    for p in range(1, PEERS):
        total = total + momrecv[p]
    slot = xl * 2 + core
    momx[slot] = total
    for who in (core_id, lo_id, diag_id):
        rcopy(momx.at[slot], momx.at[slot], q_s, q_r, who).start()
    wait_bytes(finrecv.at[pl.ds(0, PEERS - 1)], f_r)
    part = me // (PR // 2)
    for k in range(TILES):
        for j in range(CH):
            col = (j * TILES + k) * LANES
            out_ref[:, col:col + LANES] = finrecv[PARTS * k + part, 2 * j:2 * j + 2, :]
    wait_bytes(momx.at[pl.ds(0, 3)], q_r)
    moments = jnp.sum(
        (momx[0] + momx[1]) + (momx[2] + momx[3]), axis=1, keepdims=True
    ) * (1.0 / (NP * COLS * 4))
    energy = jnp.zeros((), F32)
    for k, c in enumerate(cheb_coefficients(ITERS + 1)):
        mom_out[k] = moments[k, 0]
        energy = energy + moments[k, 0] * float(c)
    energy_out[0] = energy
    wait_bytes(momrecv.at[pl.ds(0, PEERS - 1)], m_s)
    wait_bytes(finrecv.at[pl.ds(0, PEERS - 1)], f_s)
    wait_bytes(momx.at[pl.ds(0, 3)], q_s)


def per_device(pair_factors, pair_weights, probes):
    vm = pltpu.VMEM
    dma = pltpu.SemaphoreType.DMA
    out, moments, energy = pl.pallas_call(
        kernel,
        out_shape=(
            jax.ShapeDtypeStruct((2, COLS), F32),
            jax.ShapeDtypeStruct((ITERS + 1,), F32),
            jax.ShapeDtypeStruct((1,), F32),
        ),
        in_specs=[
            pl.BlockSpec(memory_space=pl.ANY),
            pl.BlockSpec(memory_space=pltpu.VMEM),
            pl.BlockSpec(memory_space=pl.ANY),
        ],
        out_specs=(
            pl.BlockSpec(memory_space=pltpu.VMEM),
            pl.BlockSpec(memory_space=pltpu.SMEM),
            pl.BlockSpec(memory_space=pltpu.SMEM),
        ),
        scratch_shapes=[
            vm((ROWS, COLS), BF16),
            vm((COLS, ROWS), BF16),
            vm((NP, COLS), F32),
            vm((CH, PEERS, PR, LANES), BF16),
            vm((NCH, NP, RCH), F32),
            vm((NCH, NP, RH), F32),
            vm((NCH, NP, RH), BF16),
            vm((NCH, NP, RH), BF16),
            vm((NCH, NP, RH), BF16),
            vm((2, NCH, NP, RH), BF16),
            vm((2 * NCH, NP, RH), BF16),
            vm((CH, PEERS, PR, LANES), BF16),
            vm((CH, PEERS, PR, LANES), BF16),
            vm((CH, PR, LANES), F32),
            vm((CH, PR, LANES), F32),
            vm((CH, PR, LANES), F32),
            vm((PR // 2, 2 * CH, LANES), F32),
            vm((PEERS, 2 * CH, LANES), F32),
            vm((16, LANES), F32),
            vm((PEERS, 16, LANES), F32),
            vm((4, 16, LANES), F32),
            dma((ROWS // 256 + 1,)),
            dma((NCH,)), dma((NCH,)),
            dma((NCH,)), dma((2, NCH)),
            dma((NCH,)), dma((NCH,)),
            dma((CH,)), dma((CH,)),
            dma((CH,)), dma((CH,)),
            dma, dma, dma, dma, dma, dma,
        ],
        compiler_params=pltpu.CompilerParams(
            collective_id=0, has_side_effects=True, vmem_limit_bytes=60 * 1024 * 1024
        ),
        name="cheb",
    )(pair_factors, pair_weights.reshape(2 * NCH, 1, RH), probes.T)
    return (out.T, moments, energy)


def solution(mesh):
    torus = Mesh(
        mesh.devices.reshape(4, 4, 2, 2, 2), ("pair_0", "pair_1", "pair_2", "aux_0", "aux_1")
    )
    return jax.shard_map(
        per_device,
        mesh=torus,
        in_specs=(P(PAIR, AUX), P(PAIR), P(AUX, None)),
        out_specs=(P(AUX, PAIR), P(), P()),
        check_vma=False,
    )
```

```python
import jax
import jax.numpy as jnp
import numpy as np
from jax import lax
from jax.experimental import pallas as pl
from jax.experimental.pallas import tpu as pltpu
from jax.sharding import Mesh
from jax.sharding import PartitionSpec as P

ITERS = 8
AUX = ("aux_0", "aux_1")
PAIR = ("pair_0", "pair_1", "pair_2")
MESH_ID = pl.DeviceIdType.MESH
F32 = jnp.float32
BF16 = jnp.bfloat16

spread = 5.0

ROWS = 2048
COLS = 4096
NP = 64
CH = 4
WIDE = COLS // CH
TILES = WIDE // 128
OWNERS = 32
PARTS = OWNERS // TILES
PR = NP // PARTS
PEERS = 32
LANES = 128
NCH = 4
RCH = ROWS // NCH
RH = RCH // 2

PLANE = (
    (2, 2), (2, 1), (2, 3), (1, 2), (3, 2), (1, 1), (3, 3), (1, 3),
    (3, 1), (2, 0), (0, 2), (1, 0), (0, 1), (3, 0), (0, 3), (0, 0),
)
OFFSETS = tuple((dy, dz, 1) for dy, dz in PLANE) + tuple((dy, dz, 0) for dy, dz in PLANE[:-1])
ZH = ((2, 1), (1, 1), (3, 1), (2, 0), (0, 1), (1, 0), (3, 0), (0, 0))


def cheb_coefficients(order_count):
    node_count = 64
    angles = (np.arange(node_count) + 0.5) * np.pi / node_count
    samples = np.log(1.0 + spread * (np.cos(angles) + 1.0) / 2.0)
    values = [
        2.0 / node_count * np.sum(samples * np.cos(degree * angles))
        for degree in range(order_count)
    ]
    values[0] = values[0] / 2.0
    return np.array(values)


def padded_dot(a, b):
    rows = a.shape[0]
    full = jnp.concatenate([a, jnp.zeros((128 - rows, a.shape[1]), a.dtype)], axis=0)
    return jnp.dot(full, b, preferred_element_type=F32)[:rows]


def kernel(
    b_hbm, w_ref, z_hbm, out_ref, mom_out, energy_out,
    bmat, bt, zbuf, vg, racc, own_half, asend, arecv, bsend, brecv, sbuf,
    rssend, rsrecv, prob, prev, cur, finsend, finrecv, mom, momrecv, momx,
    load_sem, a_s, a_r, b_s, b_r, c_s, c_r, rs_s, rs_r, ag_s, ag_r, f_s, f_r, m_s, m_r, q_s, q_r,
):
    y = lax.axis_index("pair_0")
    z = lax.axis_index("pair_1")
    h = lax.axis_index("pair_2")
    xl = lax.axis_index("aux_0")
    core = lax.axis_index("aux_1")
    me = (y * 4 + z) * 2 + h
    slot = xl * 2 + core

    def peer(dy, dz, dh):
        return {
            "pair_0": lax.rem(y + dy, 4), "pair_1": lax.rem(z + dz, 4), "pair_2": lax.rem(h + dh, 2)
        }

    def peer_index(dy, dz, dh):
        return (lax.rem(y + dy, 4) * 4 + lax.rem(z + dz, 4)) * 2 + lax.rem(h + dh, 2)

    lo_id = {"aux_0": 1 - xl}
    core_id = {"aux_1": 1 - core}
    diag_id = {"aux_0": 1 - xl, "aux_1": 1 - core}

    loads = [
        pltpu.make_async_copy(
            b_hbm.at[pl.ds(r * 256, 256)], bmat.at[pl.ds(r * 256, 256)], load_sem.at[r]
        )
        for r in range(ROWS // 256)
    ]
    zload = pltpu.make_async_copy(z_hbm, zbuf, load_sem.at[ROWS // 256])
    loads[0].start()
    zload.start()
    for ld in loads[1:]:
        ld.start()

    barrier = pltpu.get_barrier_semaphore()
    everyone = [peer(*off) for off in OFFSETS] + [lo_id, core_id, diag_id]
    for who in everyone:
        pl.semaphore_signal(barrier, inc=1, device_id=who, device_id_type=MESH_ID)

    def rcopy(src, dst, s, r, who):
        return pltpu.make_async_remote_copy(
            src_ref=src, dst_ref=dst, send_sem=s, recv_sem=r, device_id=who, device_id_type=MESH_ID
        )

    def wait_bytes(ref, sem):
        pltpu.make_async_copy(ref, ref, sem).wait()

    def flip_rows(r):
        loads[r].wait()

        def flip(k, carry):
            bt[pl.ds(k * 256, 256), r * 256:(r + 1) * 256] = bmat[
                r * 256:(r + 1) * 256, pl.ds(k * 256, 256)
            ].T
            return carry

        lax.fori_loop(0, COLS // 256, flip, 0, unroll=4)

    flip_rows(0)
    zload.wait()
    for j in range(CH):
        for p in range(PEERS):
            col = (j * TILES + p // PARTS) * LANES
            row = PR * (p % PARTS)
            vg[j, p] = zbuf[row:row + PR, col:col + LANES].astype(BF16)
        blk = zbuf[
            pl.ds(pl.multiple_of(PR * lax.rem(me, PARTS), PR), PR),
            pl.ds(pl.multiple_of((j * TILES + me // PARTS) * LANES, LANES), LANES),
        ]
        prob[j] = blk
        cur[j] = blk
        prev[j] = blk

    def dots(left):
        acc = left[0] * cur[0]
        for j in range(1, CH):
            acc = acc + left[j] * cur[j]
        return jnp.sum(acc, axis=0, keepdims=True)

    mom[...] = jnp.zeros_like(mom)
    mom[0:1, :] = dots(prob)
    def vector(j):
        return jnp.concatenate(
            [
                jnp.concatenate([vg[j, PARTS * k + g] for g in range(PARTS)], axis=0)
                for k in range(TILES)
            ],
            axis=1,
        )

    def rows_part(j, i):
        return padded_dot(
            vector(j), bt[j * WIDE:(j + 1) * WIDE, i * RCH:(i + 1) * RCH]
        )

    for r in range(1, ROWS // 256):
        flip_rows(r)
        if r % 2 == 1:
            i = r // 2
            part = rows_part(0, i)
            for j in range(1, CH - 1):
                part = part + rows_part(j, i)
            racc[i] = part

    pl.semaphore_wait(barrier, len(everyone))

    def step(t, carry):
        par = lax.rem(t, 2)

        for j in range(CH):
            @pl.when(t > 0)
            def _(j=j):
                wait_bytes(vg.at[j, pl.ds(0, PEERS - 1)], ag_r.at[j])
                if j < CH - 1:
                    for i in range(NCH):
                        part = rows_part(j, i)
                        racc[i] = part if j == 0 else racc[i] + part

        acopy = [
            rcopy(asend.at[i], arecv.at[i], a_s.at[i], a_r.at[i], core_id) for i in range(NCH)
        ]
        bcopy = [
            rcopy(bsend.at[i], brecv.at[par, i], b_s.at[i], b_r.at[par, i], lo_id)
            for i in range(NCH)
        ]
        ccopy = [
            rcopy(
                sbuf.at[2 * i + core], sbuf.at[2 * i + core], c_s.at[i], c_r.at[i], core_id
            )
            for i in range(NCH)
        ]

        def first(i):
            part = racc[i] + rows_part(CH - 1, i)
            low, high = part[:, :RH], part[:, RH:]
            own_half[i] = jnp.where(core == 0, low, high)
            asend[i] = jnp.where(core == 0, high, low).astype(BF16)
            acopy[i].start()

        def second(i):
            acopy[i].wait_recv()
            bsend[i] = (own_half[i] + arecv[i].astype(F32)).astype(BF16)
            bcopy[i].start()

        def third(i):
            bcopy[i].wait_recv()
            total = bsend[i].astype(F32) + brecv[par, i].astype(F32)
            sbuf[2 * i + core] = (w_ref[2 * i + core] * total).astype(BF16)
            ccopy[i].start()

        for i in range(NCH):
            first(i)
        for i in range(NCH):
            second(i)

        @pl.when(t > 0)
        def _():
            for j in range(CH):
                wait_bytes(vg.at[j, pl.ds(0, PEERS - 1)], ag_s.at[j])

        for i in range(NCH):
            third(i)
        for i in range(NCH):
            ccopy[i].wait_recv()

        def scaled():
            return jnp.concatenate([sbuf[q] for q in range(2 * NCH)], axis=1)

        for j in range(CH):
            for k in range(TILES // 4):
                if CH == 2:
                    side = lax.rem(y + (2, 1, 3, 0)[k], 4)
                    ys = [side]
                else:
                    side = (1 - y // 2) if k == 0 else y // 2
                    low = lax.rem(y, 2)
                    ys = [2 * side + low, 2 * side + 1 - low]
                    ys = ys if k == 0 else ys[::-1]
                col = pl.multiple_of(j * WIDE + side * 512, 512)
                img = padded_dot(scaled(), bmat[:, pl.ds(col, 512)]).astype(BF16)
                for q in range(4):
                    for g in range(PARTS):
                        rssend[j, (side * 4 + q) * PARTS + g] = img[
                            g * PR:(g + 1) * PR, q * LANES:(q + 1) * LANES
                        ]
                for m, ty in enumerate(ys):
                    own = k == TILES // 4 - 1 and m == len(ys) - 1
                    for dz, dh in ZH[:7] if own else ZH:
                        tz = lax.rem(z + dz, 4)
                        th = lax.rem(h + dh, 2)
                        rcopy(
                            rssend.at[j, (ty * 4 + tz) * 2 + th], rsrecv.at[j, me],
                            rs_s.at[j], rs_r.at[j], {"pair_0": ty, "pair_1": tz, "pair_2": th},
                        ).start()
            rsrecv[j, me] = rssend[j, me]

        @pl.when(t == ITERS - 1)
        def _():
            wait_bytes(momrecv.at[pl.ds(0, PEERS - 1)], m_r)
            total = momrecv[0]
            for p in range(1, PEERS):
                total = total + momrecv[p]
            momx[slot] = total
            for who in (core_id, lo_id, diag_id):
                rcopy(momx.at[slot], momx.at[slot], q_s, q_r, who).start()

        for i in range(NCH):
            acopy[i].wait_send()
            bcopy[i].wait_send()
            ccopy[i].wait_send()

        gain = jnp.where(t == 0, 1.0, 2.0).astype(F32)
        back = jnp.where(t == 0, 0.0, 1.0).astype(F32)
        for j in range(CH):
            wait_bytes(rsrecv.at[j, pl.ds(0, PEERS - 1)], rs_r.at[j])
            image = rsrecv[j, 0].astype(F32)
            for p in range(1, PEERS):
                image = image + rsrecv[j, p].astype(F32)
            now = cur[j]
            mapped = (2.0 / spread) * image - now
            following = gain * mapped - back * prev[j]
            prev[j] = now
            cur[j] = following

            @pl.when(t < ITERS - 1)
            def _(j=j, following=following):
                vg[j, me] = following.astype(BF16)
                for off in OFFSETS:
                    rcopy(
                        vg.at[j, me], vg.at[j, me], ag_s.at[j], ag_r.at[j], peer(*off)
                    ).start()

        @pl.when(t < ITERS - 1)
        def _():
            mom[pl.ds(t + 1, 1), :] = dots(prob)

        @pl.when(t == ITERS // 2 - 1)
        def _():
            mom[ITERS:ITERS + 1, :] = dots(cur)

        @pl.when(t == ITERS - 2)
        def _():
            momrecv[me] = mom[...]
            for off in OFFSETS:
                rcopy(mom, momrecv.at[me], m_s, m_r, peer(*off)).start()

        for j in range(CH):
            wait_bytes(rssend.at[j, pl.ds(0, PEERS - 1)], rs_s.at[j])
        return carry

    lax.fori_loop(0, ITERS, step, 0)

    for q in range(PR // 2):
        for j in range(CH):
            finsend[q, 2 * j:2 * j + 2, :] = cur[j, 2 * q:2 * q + 2, :]
    for off in OFFSETS:
        rcopy(
            finsend.at[lax.rem(peer_index(*off), PR // 2)], finrecv.at[me], f_s, f_r, peer(*off)
        ).start()
    finrecv[me] = finsend[lax.rem(me, PR // 2)]

    wait_bytes(momx.at[pl.ds(0, 3)], q_r)
    moments = jnp.sum(
        (momx[0] + momx[1]) + (momx[2] + momx[3]), axis=1, keepdims=True
    ) * (1.0 / (NP * COLS * 4))
    energy = jnp.zeros((), F32)
    for k, c in enumerate(cheb_coefficients(ITERS + 1)):
        value = moments[k, 0] if k < ITERS else 2.0 * moments[k, 0] - moments[0, 0]
        mom_out[k] = value
        energy = energy + value * float(c)
    energy_out[0] = energy
    wait_bytes(finrecv.at[pl.ds(0, PEERS - 1)], f_r)
    part = me // (PR // 2)
    for k in range(TILES):
        for j in range(CH):
            col = (j * TILES + k) * LANES
            out_ref[:, col:col + LANES] = finrecv[PARTS * k + part, 2 * j:2 * j + 2, :]
    wait_bytes(momrecv.at[pl.ds(0, PEERS - 1)], m_s)
    wait_bytes(finrecv.at[pl.ds(0, PEERS - 1)], f_s)
    wait_bytes(momx.at[pl.ds(0, 3)], q_s)


def per_device(pair_factors, pair_weights, probes):
    vm = pltpu.VMEM
    dma = pltpu.SemaphoreType.DMA
    out, moments, energy = pl.pallas_call(
        kernel,
        out_shape=(
            jax.ShapeDtypeStruct((2, COLS), F32),
            jax.ShapeDtypeStruct((ITERS + 1,), F32),
            jax.ShapeDtypeStruct((1,), F32),
        ),
        in_specs=[
            pl.BlockSpec(memory_space=pl.ANY),
            pl.BlockSpec(memory_space=pltpu.VMEM),
            pl.BlockSpec(memory_space=pl.ANY),
        ],
        out_specs=(
            pl.BlockSpec(memory_space=pltpu.VMEM),
            pl.BlockSpec(memory_space=pltpu.SMEM),
            pl.BlockSpec(memory_space=pltpu.SMEM),
        ),
        scratch_shapes=[
            vm((ROWS, COLS), BF16),
            vm((COLS, ROWS), BF16),
            vm((NP, COLS), F32),
            vm((CH, PEERS, PR, LANES), BF16),
            vm((NCH, NP, RCH), F32),
            vm((NCH, NP, RH), F32),
            vm((NCH, NP, RH), BF16),
            vm((NCH, NP, RH), BF16),
            vm((NCH, NP, RH), BF16),
            vm((2, NCH, NP, RH), BF16),
            vm((2 * NCH, NP, RH), BF16),
            vm((CH, PEERS, PR, LANES), BF16),
            vm((CH, PEERS, PR, LANES), BF16),
            vm((CH, PR, LANES), F32),
            vm((CH, PR, LANES), F32),
            vm((CH, PR, LANES), F32),
            vm((PR // 2, 2 * CH, LANES), F32),
            vm((PEERS, 2 * CH, LANES), F32),
            vm((16, LANES), F32),
            vm((PEERS, 16, LANES), F32),
            vm((4, 16, LANES), F32),
            dma((ROWS // 256 + 1,)),
            dma((NCH,)), dma((NCH,)),
            dma((NCH,)), dma((2, NCH)),
            dma((NCH,)), dma((NCH,)),
            dma((CH,)), dma((CH,)),
            dma((CH,)), dma((CH,)),
            dma, dma, dma, dma, dma, dma,
        ],
        compiler_params=pltpu.CompilerParams(
            collective_id=0, has_side_effects=True, vmem_limit_bytes=60 * 1024 * 1024
        ),
        name="cheb",
    )(pair_factors, pair_weights.reshape(2 * NCH, 1, RH), probes.T)
    return (out.T, moments, energy)


def solution(mesh):
    torus = Mesh(
        mesh.devices.reshape(4, 4, 2, 2, 2), ("pair_0", "pair_1", "pair_2", "aux_0", "aux_1")
    )
    return jax.shard_map(
        per_device,
        mesh=torus,
        in_specs=(P(PAIR, AUX), P(PAIR), P(AUX, None)),
        out_specs=(P(AUX, PAIR), P(), P()),
        check_vma=False,
    )
```

```python
import jax
import jax.numpy as jnp
import numpy as np
from jax import lax
from jax.experimental import pallas as pl
from jax.experimental.pallas import tpu as pltpu
from jax.sharding import Mesh
from jax.sharding import PartitionSpec as P

ITERS = 8
AUX = ("aux_0", "aux_1")
PAIR = ("pair_0", "pair_1", "pair_2")
MESH_ID = pl.DeviceIdType.MESH
F32 = jnp.float32
BF16 = jnp.bfloat16

spread = 5.0

ROWS = 2048
COLS = 4096
NP = 64
CH = 4
WIDE = COLS // CH
TILES = WIDE // 128
OWNERS = 32
PARTS = OWNERS // TILES
PR = NP // PARTS
PEERS = 32
LANES = 128
NCH = 4
RCH = ROWS // NCH
RH = RCH // 2

PLANE = (
    (2, 2), (2, 1), (2, 3), (1, 2), (3, 2), (1, 1), (3, 3), (1, 3),
    (3, 1), (2, 0), (0, 2), (1, 0), (0, 1), (3, 0), (0, 3), (0, 0),
)
OFFSETS = tuple((dy, dz, 1) for dy, dz in PLANE) + tuple((dy, dz, 0) for dy, dz in PLANE[:-1])
ZH = ((2, 1), (1, 1), (3, 1), (2, 0), (0, 1), (1, 0), (3, 0), (0, 0))


def cheb_coefficients(order_count):
    node_count = 64
    angles = (np.arange(node_count) + 0.5) * np.pi / node_count
    samples = np.log(1.0 + spread * (np.cos(angles) + 1.0) / 2.0)
    values = [
        2.0 / node_count * np.sum(samples * np.cos(degree * angles))
        for degree in range(order_count)
    ]
    values[0] = values[0] / 2.0
    return np.array(values)


def padded_dot(a, b):
    rows = a.shape[0]
    full = jnp.concatenate([a, jnp.zeros((128 - rows, a.shape[1]), a.dtype)], axis=0)
    return jnp.dot(full, b, preferred_element_type=F32)[:rows]


def kernel(
    b_hbm, w_ref, z_hbm, out_ref, mom_out, energy_out,
    bmat, bt, zbuf, vg, racc, iacc, own_half, asend, arecv, bsend, brecv, sbuf,
    rssend, rsrecv, prob, prev, cur, finsend, finrecv, mom, momrecv, momx,
    load_sem, a_s, a_r, b_s, b_r, c_s, c_r, rs_s, rs_r, ag_s, ag_r, f_s, f_r, m_s, m_r, q_s, q_r,
):
    y = lax.axis_index("pair_0")
    z = lax.axis_index("pair_1")
    h = lax.axis_index("pair_2")
    xl = lax.axis_index("aux_0")
    core = lax.axis_index("aux_1")
    me = (y * 4 + z) * 2 + h
    slot = xl * 2 + core

    def peer(dy, dz, dh):
        return {
            "pair_0": lax.rem(y + dy, 4), "pair_1": lax.rem(z + dz, 4), "pair_2": lax.rem(h + dh, 2)
        }

    def peer_index(dy, dz, dh):
        return (lax.rem(y + dy, 4) * 4 + lax.rem(z + dz, 4)) * 2 + lax.rem(h + dh, 2)

    lo_id = {"aux_0": 1 - xl}
    core_id = {"aux_1": 1 - core}
    diag_id = {"aux_0": 1 - xl, "aux_1": 1 - core}

    loads = [
        pltpu.make_async_copy(
            b_hbm.at[pl.ds(r * 256, 256)], bmat.at[pl.ds(r * 256, 256)], load_sem.at[r]
        )
        for r in range(ROWS // 256)
    ]
    zload = pltpu.make_async_copy(z_hbm, zbuf, load_sem.at[ROWS // 256])
    loads[0].start()
    zload.start()
    for ld in loads[1:]:
        ld.start()

    barrier = pltpu.get_barrier_semaphore()
    everyone = [peer(*off) for off in OFFSETS] + [lo_id, core_id, diag_id]
    for who in everyone:
        pl.semaphore_signal(barrier, inc=1, device_id=who, device_id_type=MESH_ID)

    def rcopy(src, dst, s, r, who):
        return pltpu.make_async_remote_copy(
            src_ref=src, dst_ref=dst, send_sem=s, recv_sem=r, device_id=who, device_id_type=MESH_ID
        )

    def wait_bytes(ref, sem):
        pltpu.make_async_copy(ref, ref, sem).wait()

    def flip_rows(r):
        loads[r].wait()

        def flip(k, carry):
            bt[pl.ds(k * 256, 256), r * 256:(r + 1) * 256] = bmat[
                r * 256:(r + 1) * 256, pl.ds(k * 256, 256)
            ].T
            return carry

        lax.fori_loop(0, COLS // 256, flip, 0, unroll=4)

    flip_rows(0)
    zload.wait()
    for j in range(CH):
        for p in range(PEERS):
            col = (j * TILES + p // PARTS) * LANES
            row = PR * (p % PARTS)
            vg[j, p] = zbuf[row:row + PR, col:col + LANES].astype(BF16)
        blk = zbuf[
            pl.ds(pl.multiple_of(PR * lax.rem(me, PARTS), PR), PR),
            pl.ds(pl.multiple_of((j * TILES + me // PARTS) * LANES, LANES), LANES),
        ]
        prob[j] = blk
        cur[j] = blk
        prev[j] = blk

    def dots(left):
        acc = left[0] * cur[0]
        for j in range(1, CH):
            acc = acc + left[j] * cur[j]
        return jnp.sum(acc, axis=0, keepdims=True)

    mom[...] = jnp.zeros_like(mom)
    mom[0:1, :] = dots(prob)
    def vector(j):
        return jnp.concatenate(
            [
                jnp.concatenate([vg[j, PARTS * k + g] for g in range(PARTS)], axis=0)
                for k in range(TILES)
            ],
            axis=1,
        )

    def rows_part(j, i):
        return padded_dot(
            vector(j), bt[j * WIDE:(j + 1) * WIDE, i * RCH:(i + 1) * RCH]
        )

    for r in range(1, ROWS // 256):
        flip_rows(r)
        if r % 2 == 1:
            i = r // 2
            part = rows_part(0, i)
            for j in range(1, CH - 1):
                part = part + rows_part(j, i)
            racc[i] = part

    pl.semaphore_wait(barrier, len(everyone))

    def step(t, carry):
        par = lax.rem(t, 2)

        for j in range(CH):
            @pl.when(t > 0)
            def _(j=j):
                wait_bytes(vg.at[j, pl.ds(0, PEERS - 1)], ag_r.at[j])
                if j < CH - 1:
                    for i in range(NCH):
                        part = rows_part(j, i)
                        racc[i] = part if j == 0 else racc[i] + part

        acopy = [
            rcopy(asend.at[i], arecv.at[i], a_s.at[i], a_r.at[i], core_id) for i in range(NCH)
        ]
        bcopy = [
            rcopy(bsend.at[i], brecv.at[par, i], b_s.at[i], b_r.at[par, i], lo_id)
            for i in range(NCH)
        ]
        ccopy = [
            rcopy(
                sbuf.at[2 * i + core], sbuf.at[2 * i + core], c_s.at[i], c_r.at[i], core_id
            )
            for i in range(NCH)
        ]

        def first(i):
            part = racc[i] + rows_part(CH - 1, i)
            low, high = part[:, :RH], part[:, RH:]
            own_half[i] = jnp.where(core == 0, low, high)
            asend[i] = jnp.where(core == 0, high, low).astype(BF16)
            acopy[i].start()

        def second(i):
            acopy[i].wait_recv()
            bsend[i] = (own_half[i] + arecv[i].astype(F32)).astype(BF16)
            bcopy[i].start()

        def third(i):
            bcopy[i].wait_recv()
            total = bsend[i].astype(F32) + brecv[par, i].astype(F32)
            sbuf[2 * i + core] = (w_ref[2 * i + core] * total).astype(BF16)
            ccopy[i].start()

        for i in range(NCH):
            first(i)
        for i in range(NCH):
            second(i)

        @pl.when(t > 0)
        def _():
            for j in range(CH):
                wait_bytes(vg.at[j, pl.ds(0, PEERS - 1)], ag_s.at[j])

        for i in range(NCH):
            third(i)
        def half_image(who, col):
            pieces = [bmat[pl.ds(pl.multiple_of((2 * i + who) * RH, RH), RH), pl.ds(col, 512)] for i in range(NCH)]
            left = jnp.concatenate([sbuf[2 * i + who] for i in range(NCH)], axis=1)
            return padded_dot(left, jnp.concatenate(pieces, axis=0))

        for n in range(COLS // 512):
            iacc[n] = half_image(core, n * 512)

        for i in range(NCH):
            ccopy[i].wait_recv()

        for j in range(CH):
            for k in range(TILES // 4):
                if CH == 2:
                    side = lax.rem(y + (2, 1, 3, 0)[k], 4)
                    ys = [side]
                else:
                    side = (1 - y // 2) if k == 0 else y // 2
                    low = lax.rem(y, 2)
                    ys = [2 * side + low, 2 * side + 1 - low]
                    ys = ys if k == 0 else ys[::-1]
                col = pl.multiple_of(j * WIDE + side * 512, 512)
                img = (iacc[j * (WIDE // 512) + side] + half_image(1 - core, col)).astype(BF16)
                for q in range(4):
                    for g in range(PARTS):
                        rssend[j, (side * 4 + q) * PARTS + g] = img[
                            g * PR:(g + 1) * PR, q * LANES:(q + 1) * LANES
                        ]
                for m, ty in enumerate(ys):
                    own = k == TILES // 4 - 1 and m == len(ys) - 1
                    for dz, dh in ZH[:7] if own else ZH:
                        tz = lax.rem(z + dz, 4)
                        th = lax.rem(h + dh, 2)
                        rcopy(
                            rssend.at[j, (ty * 4 + tz) * 2 + th], rsrecv.at[j, me],
                            rs_s.at[j], rs_r.at[j], {"pair_0": ty, "pair_1": tz, "pair_2": th},
                        ).start()
            rsrecv[j, me] = rssend[j, me]

        @pl.when(t == ITERS - 1)
        def _():
            wait_bytes(momrecv.at[pl.ds(0, PEERS - 1)], m_r)
            total = momrecv[0]
            for p in range(1, PEERS):
                total = total + momrecv[p]
            momx[slot] = total
            for who in (core_id, lo_id, diag_id):
                rcopy(momx.at[slot], momx.at[slot], q_s, q_r, who).start()

        for i in range(NCH):
            acopy[i].wait_send()
            bcopy[i].wait_send()
            ccopy[i].wait_send()

        gain = jnp.where(t == 0, 1.0, 2.0).astype(F32)
        back = jnp.where(t == 0, 0.0, 1.0).astype(F32)
        for j in range(CH):
            wait_bytes(rsrecv.at[j, pl.ds(0, PEERS - 1)], rs_r.at[j])
            image = rsrecv[j, 0].astype(F32)
            for p in range(1, PEERS):
                image = image + rsrecv[j, p].astype(F32)
            now = cur[j]
            mapped = (2.0 / spread) * image - now
            following = gain * mapped - back * prev[j]
            prev[j] = now
            cur[j] = following

            @pl.when(t < ITERS - 1)
            def _(j=j, following=following):
                vg[j, me] = following.astype(BF16)
                for off in OFFSETS:
                    rcopy(
                        vg.at[j, me], vg.at[j, me], ag_s.at[j], ag_r.at[j], peer(*off)
                    ).start()

        @pl.when(t < ITERS - 1)
        def _():
            mom[pl.ds(t + 1, 1), :] = dots(prob)

        @pl.when(t == ITERS // 2 - 1)
        def _():
            mom[ITERS:ITERS + 1, :] = dots(cur)

        @pl.when(t == ITERS - 2)
        def _():
            momrecv[me] = mom[...]
            for off in OFFSETS:
                rcopy(mom, momrecv.at[me], m_s, m_r, peer(*off)).start()

        for j in range(CH):
            wait_bytes(rssend.at[j, pl.ds(0, PEERS - 1)], rs_s.at[j])
        return carry

    lax.fori_loop(0, ITERS, step, 0)

    for q in range(PR // 2):
        for j in range(CH):
            finsend[q, 2 * j:2 * j + 2, :] = cur[j, 2 * q:2 * q + 2, :]
    for off in OFFSETS:
        rcopy(
            finsend.at[lax.rem(peer_index(*off), PR // 2)], finrecv.at[me], f_s, f_r, peer(*off)
        ).start()
    finrecv[me] = finsend[lax.rem(me, PR // 2)]

    wait_bytes(momx.at[pl.ds(0, 3)], q_r)
    moments = jnp.sum(
        (momx[0] + momx[1]) + (momx[2] + momx[3]), axis=1, keepdims=True
    ) * (1.0 / (NP * COLS * 4))
    energy = jnp.zeros((), F32)
    for k, c in enumerate(cheb_coefficients(ITERS + 1)):
        value = moments[k, 0] if k < ITERS else 2.0 * moments[k, 0] - moments[0, 0]
        mom_out[k] = value
        energy = energy + value * float(c)
    energy_out[0] = energy
    wait_bytes(finrecv.at[pl.ds(0, PEERS - 1)], f_r)
    part = me // (PR // 2)
    for k in range(TILES):
        for j in range(CH):
            col = (j * TILES + k) * LANES
            out_ref[:, col:col + LANES] = finrecv[PARTS * k + part, 2 * j:2 * j + 2, :]
    wait_bytes(momrecv.at[pl.ds(0, PEERS - 1)], m_s)
    wait_bytes(finrecv.at[pl.ds(0, PEERS - 1)], f_s)
    wait_bytes(momx.at[pl.ds(0, 3)], q_s)


def per_device(pair_factors, pair_weights, probes):
    vm = pltpu.VMEM
    dma = pltpu.SemaphoreType.DMA
    out, moments, energy = pl.pallas_call(
        kernel,
        out_shape=(
            jax.ShapeDtypeStruct((2, COLS), F32),
            jax.ShapeDtypeStruct((ITERS + 1,), F32),
            jax.ShapeDtypeStruct((1,), F32),
        ),
        in_specs=[
            pl.BlockSpec(memory_space=pl.ANY),
            pl.BlockSpec(memory_space=pltpu.VMEM),
            pl.BlockSpec(memory_space=pl.ANY),
        ],
        out_specs=(
            pl.BlockSpec(memory_space=pltpu.VMEM),
            pl.BlockSpec(memory_space=pltpu.SMEM),
            pl.BlockSpec(memory_space=pltpu.SMEM),
        ),
        scratch_shapes=[
            vm((ROWS, COLS), BF16),
            vm((COLS, ROWS), BF16),
            vm((NP, COLS), F32),
            vm((CH, PEERS, PR, LANES), BF16),
            vm((NCH, NP, RCH), F32),
            vm((COLS // 512, NP, 512), F32),
            vm((NCH, NP, RH), F32),
            vm((NCH, NP, RH), BF16),
            vm((NCH, NP, RH), BF16),
            vm((NCH, NP, RH), BF16),
            vm((2, NCH, NP, RH), BF16),
            vm((2 * NCH, NP, RH), BF16),
            vm((CH, PEERS, PR, LANES), BF16),
            vm((CH, PEERS, PR, LANES), BF16),
            vm((CH, PR, LANES), F32),
            vm((CH, PR, LANES), F32),
            vm((CH, PR, LANES), F32),
            vm((PR // 2, 2 * CH, LANES), F32),
            vm((PEERS, 2 * CH, LANES), F32),
            vm((16, LANES), F32),
            vm((PEERS, 16, LANES), F32),
            vm((4, 16, LANES), F32),
            dma((ROWS // 256 + 1,)),
            dma((NCH,)), dma((NCH,)),
            dma((NCH,)), dma((2, NCH)),
            dma((NCH,)), dma((NCH,)),
            dma((CH,)), dma((CH,)),
            dma((CH,)), dma((CH,)),
            dma, dma, dma, dma, dma, dma,
        ],
        compiler_params=pltpu.CompilerParams(
            collective_id=0, has_side_effects=True, vmem_limit_bytes=60 * 1024 * 1024
        ),
        name="cheb",
    )(pair_factors, pair_weights.reshape(2 * NCH, 1, RH), probes.T)
    return (out.T, moments, energy)


def solution(mesh):
    torus = Mesh(
        mesh.devices.reshape(4, 4, 2, 2, 2), ("pair_0", "pair_1", "pair_2", "aux_0", "aux_1")
    )
    return jax.shard_map(
        per_device,
        mesh=torus,
        in_specs=(P(PAIR, AUX), P(PAIR), P(AUX, None)),
        out_specs=(P(AUX, PAIR), P(), P()),
        check_vma=False,
    )
```
